32 devices in a mesh: ta: 4 (over y, core), gx: 2 (over x), gy: 4 (over z).
Axes of the slice: x: 2, y: 2, z: 4, core: 2. Of those that a mesh axis runs over, the one named last changes fastest.
Arguments:
- space_links: float32 [3, 2, 3, 3, 4, 4, 2304], P(None, None, None, None, 'ta', 'gx', 'gy'), may hold values from -1 to 1, as said below
- time_links: float32 [2, 3, 3, 4, 4, 2304], P(None, None, None, 'ta', 'gx', 'gy'), may hold values from -1 to 1, as said below
- start_gauge: float32 [2, 3, 3, 4, 4, 2304], P(None, None, None, 'ta', 'gx', 'gy'), may hold values from -1 to 1, as said below
Outputs:
- gauge_field: float32 [2, 3, 3, 4, 4, 2304], P(None, None, None, 'ta', 'gx', 'gy')
- time_rotated: float32 [2, 3, 3, 4, 4, 2304], P(None, None, None, 'ta', 'gx', 'gy')
- functional: float32 [4, 4], P(None, 'ta')
- theta: float32 [4], P('ta')
The draws below stay inside these ranges and needn't reach their ends.
Inputs may be any that keep to these rules, and one draw needn't show every extreme that they name: `space_links`: at every site the matrix is special unitary. `time_links`: at every site the matrix is special unitary. `start_gauge`: at every site the matrix is special unitary.
All inputs are finite; a program needn't handle non-finite values.
Results may differ from the reference program's by a relative error of at most 0.00021.
Values sent between devices are 32-bit elements; how exact they have to be, the bound alone decides.
A program may use at most 64 MiB of HBM per device.

```python
import jax
import jax.numpy as jnp
from jax import lax

NZ = 48
ITERS = 4
NT = 4
NX = 4
NY = 48


PAIRS = ((0, 1), (1, 2), (0, 2))


SMALL = 1e-12


def turn_rows(matrix, row_one, row_two, coeffs):
    first_re, first_im = (matrix[0, row_one], matrix[1, row_one])
    second_re, second_im = (matrix[0, row_two], matrix[1, row_two])

    def scaled(real_part, imag_part, vec_re, vec_im):
        return (real_part * vec_re - imag_part * vec_im, real_part * vec_im + imag_part * vec_re)
    one_a = scaled(coeffs[0], coeffs[3], first_re, first_im)
    one_b = scaled(coeffs[2], coeffs[1], second_re, second_im)
    two_a = scaled(-coeffs[2], coeffs[1], first_re, first_im)
    two_b = scaled(coeffs[0], -coeffs[3], second_re, second_im)
    real_new = matrix[0].at[row_one].set(one_a[0] + one_b[0]).at[row_two].set(two_a[0] + two_b[0])
    imag_new = matrix[1].at[row_one].set(one_a[1] + one_b[1]).at[row_two].set(two_a[1] + two_b[1])
    return jnp.stack([real_new, imag_new])


def unitary_near(key, site_shape, spread):
    identity = jnp.eye(3, dtype=jnp.float32).reshape((3, 3) + (1,) * len(site_shape))
    real_part = jnp.broadcast_to(identity, (3, 3) + site_shape)
    matrix = jnp.stack([real_part, jnp.zeros_like(real_part)])
    for number in range(6):
        row_one, row_two = PAIRS[number % 3]
        noise = jax.random.normal(jax.random.fold_in(key, number), (4,) + site_shape, jnp.float32)
        quaternion = [1.0 + spread * noise[0], spread * noise[1], spread * noise[2], spread * noise[3]]
        length = jnp.sqrt(quaternion[0] * quaternion[0] + quaternion[1] * quaternion[1] + quaternion[2] * quaternion[2] + quaternion[3] * quaternion[3] + SMALL)
        coeffs = [entry / length for entry in quaternion]
        matrix = turn_rows(matrix, row_one, row_two, coeffs)
    return matrix


def ramp(low_end, high_end, flipped):
    x_coord = jnp.arange(NX).astype(jnp.float32) / NX
    y_coord = (jnp.arange(NY * NZ) // NZ).astype(jnp.float32) / NY
    level = (x_coord[:, None] + y_coord[None, :]) / 2.0
    if flipped:
        level = 1.0 - level
    return low_end + (high_end - low_end) * level


def draw_space_links(key, part):
    spread = ramp(0.1, 1.1, False)
    field = unitary_near(jax.random.fold_in(key, 11), (3, NT, NX, NY * NZ), spread)
    return jnp.moveaxis(field, 3, 0)


def draw_time_links(key, part):
    spread = 0.8
    return unitary_near(jax.random.fold_in(key, 23), (NT, NX, NY * NZ), spread)


def draw_start_gauge(key, part):
    spread = ramp(0.1, 1.6, True)
    return unitary_near(jax.random.fold_in(key, 37), (NT, NX, NY * NZ), spread)


def setup_inputs(seed: int = 0) -> dict:
    arg_keys = jax.random.split(jax.random.key(seed), 4)
    space_links = draw_space_links(jax.random.fold_in(arg_keys[3], 71), 0)
    time_links = draw_time_links(jax.random.fold_in(arg_keys[3], 71), 0)
    start_gauge = draw_start_gauge(jax.random.fold_in(arg_keys[3], 71), 0)
    return {"space_links": space_links, "time_links": time_links, "start_gauge": start_gauge}


OMEGA = 1.7
FLOOR = 0.5
PAIRS = ((0, 1), (1, 2), (0, 2))

def multiply(first, second):
    return lax.optimization_barrier(jnp.sum(first[:, :, None] * second[None, :, :], axis=1))

def product(left, right):
    return jnp.stack([multiply(left[0], right[0]) - multiply(left[1], right[1]), multiply(left[0], right[1]) + multiply(left[1], right[0])])

def dagger(matrix):
    return jnp.stack([jnp.swapaxes(matrix[0], 0, 1), -jnp.swapaxes(matrix[1], 0, 1)])

def z_ahead(field, z_index):
    return jnp.where(z_index == NZ - 1, jnp.roll(field, NZ - 1, axis=-1), jnp.roll(field, -1, axis=-1))

def z_behind(field, z_index):
    return jnp.where(z_index == 0, jnp.roll(field, -(NZ - 1), axis=-1), jnp.roll(field, 1, axis=-1))

def staples(links_now, back_links, forward, backward):
    staple_sum = jnp.zeros_like(forward[0])
    for direction in range(3):
        staple_sum = staple_sum + product(links_now[direction], dagger(forward[direction]))
        staple_sum = staple_sum + product(back_links[direction], dagger(backward[direction]))
    return staple_sum

def rotate_rows(matrix, row_one, row_two, coeffs):
    first_re, first_im = (matrix[0, row_one], matrix[1, row_one])
    second_re, second_im = (matrix[0, row_two], matrix[1, row_two])

    def scaled(real_part, imag_part, vec_re, vec_im):
        return (real_part * vec_re - imag_part * vec_im, real_part * vec_im + imag_part * vec_re)
    one_a = scaled(coeffs[0], coeffs[3], first_re, first_im)
    one_b = scaled(coeffs[2], coeffs[1], second_re, second_im)
    two_a = scaled(-coeffs[2], coeffs[1], first_re, first_im)
    two_b = scaled(coeffs[0], -coeffs[3], second_re, second_im)
    real_new = matrix[0].at[row_one].set(one_a[0] + one_b[0]).at[row_two].set(two_a[0] + two_b[0])
    imag_new = matrix[1].at[row_one].set(one_a[1] + one_b[1]).at[row_two].set(two_a[1] + two_b[1])
    return jnp.stack([real_new, imag_new])

def relax_sites(gauge_field, staple_sum, chosen):
    moment = product(gauge_field, staple_sum)
    candidate = gauge_field
    for row_one, row_two in PAIRS:
        vector = [moment[0, row_one, row_one] + moment[0, row_two, row_two], -(moment[1, row_one, row_two] + moment[1, row_two, row_one]), moment[0, row_two, row_one] - moment[0, row_one, row_two], moment[1, row_two, row_two] - moment[1, row_one, row_one]]
        length = jnp.sqrt(vector[0] * vector[0] + vector[1] * vector[1] + vector[2] * vector[2] + vector[3] * vector[3])
        pushed = [(1.0 - OMEGA) * length + OMEGA * vector[0], OMEGA * vector[1], OMEGA * vector[2], OMEGA * vector[3]]
        inverse = 1.0 / jnp.maximum(jnp.sqrt(pushed[0] * pushed[0] + pushed[1] * pushed[1] + pushed[2] * pushed[2] + pushed[3] * pushed[3]), FLOOR)
        coeffs = [entry * inverse for entry in pushed]
        candidate = rotate_rows(candidate, row_one, row_two, coeffs)
        moment = rotate_rows(moment, row_one, row_two, coeffs)
    trace_re = moment[0, 0, 0] + moment[0, 1, 1] + moment[0, 2, 2]
    return (jnp.where(chosen, candidate, gauge_field), jnp.where(chosen, trace_re, 0.0))

def antihermitian(matrix):
    half = (matrix - dagger(matrix)) / 2.0
    trace_im = half[1, 0, 0] + half[1, 1, 1] + half[1, 2, 2]
    identity = jnp.eye(3, dtype=matrix.dtype).reshape((3, 3) + (1,) * (matrix.ndim - 3))
    return jnp.stack([half[0], half[1] - identity * (trace_im / 3.0)])

def divergence_squares(gauge_field, links_now, lower_links, forward, backward):
    delta = jnp.zeros_like(gauge_field)
    for direction in range(3):
        here = product(product(gauge_field, links_now[direction]), dagger(forward[direction]))
        there = product(product(backward[direction], lower_links[direction]), dagger(gauge_field))
        delta = delta + antihermitian(there) - antihermitian(here)
    return lax.optimization_barrier(jnp.sum(delta * delta, axis=(0, 1, 2)))

def reference(space_links, time_links, start_gauge):
    x_count = space_links.shape[-2]
    row_width = space_links.shape[-1]
    volume = x_count * row_width
    z_index = jnp.arange(row_width) % NZ
    parity = (jnp.arange(x_count)[:, None] + (jnp.arange(row_width) // NZ)[None, :] + z_index[None, :]) % 2

    def neighbours(gauge_field):
        forward = [jnp.roll(gauge_field, -1, axis=-2), jnp.roll(gauge_field, -NZ, axis=-1), z_ahead(gauge_field, z_index)]
        backward = [jnp.roll(gauge_field, 1, axis=-2), jnp.roll(gauge_field, NZ, axis=-1), z_behind(gauge_field, z_index)]
        return (forward, backward)

    def fix_slice(inputs):
        links_now, gauge_field = inputs
        lower_links = [jnp.roll(links_now[0], 1, axis=-2), jnp.roll(links_now[1], NZ, axis=-1), z_behind(links_now[2], z_index)]
        back_links = [dagger(lower_link) for lower_link in lower_links]
        scores = []
        for iteration in range(ITERS):
            for colour in (0, 1):
                forward, backward = neighbours(gauge_field)
                staple_sum = staples(links_now, back_links, forward, backward)
                gauge_field, local_terms = relax_sites(gauge_field, staple_sum, parity == colour)
            scores.append(jnp.sum(local_terms) / (9.0 * volume))
        forward, backward = neighbours(gauge_field)
        theta_value = jnp.sum(divergence_squares(gauge_field, links_now, lower_links, forward, backward)) / (3.0 * volume)
        return (gauge_field, jnp.stack(scores), theta_value)
    gauges, scores, theta = lax.map(fix_slice, (jnp.moveaxis(space_links, 4, 0), jnp.moveaxis(start_gauge, 3, 0)))
    following = jnp.roll(gauges, -1, axis=0)

    def rotate_time(inputs):
        here, link_now, ahead_gauge = inputs
        return product(product(here, link_now), dagger(ahead_gauge))
    rotated = lax.map(rotate_time, (gauges, jnp.moveaxis(time_links, 3, 0), following))
    return (jnp.moveaxis(gauges, 0, 3), jnp.moveaxis(rotated, 0, 3), jnp.transpose(scores), theta)
```

```python
import functools

import jax
import jax.numpy as jnp
from jax import lax
from jax.experimental import pallas as pl
from jax.experimental.pallas import tpu as pltpu
from jax.sharding import PartitionSpec as P

NZ = 48
ITERS = 4
OMEGA = 1.7
FLOOR = 0.5
PAIRS = ((0, 1), (1, 2), (0, 2))

COMPS = 72
GAUGE = 54
MESH = pl.DeviceIdType.MESH


def tile(ref, row):
    return ref[pl.ds(row * 8, 8), :]


def z_shift(v, masks, step):
    lane, z = masks
    if step > 0:
        return jnp.where(z == NZ - 1, pltpu.roll(v, NZ - 1, 1), pltpu.roll(v, 127, 1))
    return jnp.where(z == 0, pltpu.roll(v, 128 - (NZ - 1), 1), pltpu.roll(v, 1, 1))


def y_shift(v, masks, step):
    lane, z = masks
    swapped = pltpu.roll(v, 64, 1)
    if step > 0:
        return jnp.where(lane < 64, swapped, pltpu.roll(swapped, 7, 0))
    return jnp.where(lane >= 64, swapped, pltpu.roll(swapped, 1, 0))


def add_links_times_dagger(total, u, g):
    for i in range(3):
        for j in range(3):
            re, im = total[i * 3 + j], total[9 + i * 3 + j]
            for k in range(3):
                ur, ui = u[i * 3 + k], u[9 + i * 3 + k]
                gr, gi = g[j * 3 + k], g[9 + j * 3 + k]
                tr = ur * gr + ui * gi
                ti = ui * gr - ur * gi
                re = tr if re is None else re + tr
                im = ti if im is None else im + ti
            total[i * 3 + j], total[9 + i * 3 + j] = re, im


def add_dagger_times_dagger(total, v, g):
    for i in range(3):
        for j in range(3):
            re, im = total[i * 3 + j], total[9 + i * 3 + j]
            for k in range(3):
                vr, vi = v[k * 3 + i], v[9 + k * 3 + i]
                gr, gi = g[j * 3 + k], g[9 + j * 3 + k]
                tr = vr * gr - vi * gi
                ti = vr * gi + vi * gr
                re = tr if re is None else re + tr
                im = -ti if im is None else im - ti
            total[i * 3 + j], total[9 + i * 3 + j] = re, im


def times(a, b):
    out = [None] * 18
    for i in range(3):
        for j in range(3):
            re = im = None
            for k in range(3):
                ar, ai = a[i * 3 + k], a[9 + i * 3 + k]
                br, bi = b[k * 3 + j], b[9 + k * 3 + j]
                tr = ar * br - ai * bi
                ti = ar * bi + ai * br
                re = tr if re is None else re + tr
                im = ti if im is None else im + ti
            out[i * 3 + j], out[9 + i * 3 + j] = re, im
    return out


def turn(m, i, j, a):
    out = list(m)
    for col in range(3):
        fr, fi = m[i * 3 + col], m[9 + i * 3 + col]
        sr, si = m[j * 3 + col], m[9 + j * 3 + col]
        out[i * 3 + col] = (a[0] * fr - a[3] * fi) + (a[2] * sr - a[1] * si)
        out[9 + i * 3 + col] = (a[0] * fi + a[3] * fr) + (a[2] * si + a[1] * sr)
        out[j * 3 + col] = (a[0] * sr + a[3] * si) - (a[2] * fr + a[1] * fi)
        out[9 + j * 3 + col] = (a[0] * si - a[3] * sr) - (a[2] * fi - a[1] * fr)
    return out


def relax(g, m):
    for i, j in PAIRS:
        c0 = m[i * 3 + i] + m[j * 3 + j]
        c1 = -(m[9 + i * 3 + j] + m[9 + j * 3 + i])
        c2 = m[j * 3 + i] - m[i * 3 + j]
        c3 = m[9 + j * 3 + j] - m[9 + i * 3 + i]
        length = jnp.sqrt(c0 * c0 + c1 * c1 + c2 * c2 + c3 * c3)
        v0 = (1.0 - OMEGA) * length + OMEGA * c0
        v1, v2, v3 = OMEGA * c1, OMEGA * c2, OMEGA * c3
        inverse = jnp.minimum(lax.rsqrt(v0 * v0 + v1 * v1 + v2 * v2 + v3 * v3), 1.0 / FLOOR)
        a = [v0 * inverse, v1 * inverse, v2 * inverse, v3 * inverse]
        g = turn(g, i, j, a)
        m = turn(m, i, j, a)
    return g, m


def squares(m):
    total = None
    for i, j in ((0, 1), (0, 2), (1, 2)):
        a = m[i * 3 + j] - m[j * 3 + i]
        b = m[9 + i * 3 + j] + m[9 + j * 3 + i]
        term = 0.5 * (a * a + b * b)
        total = term if total is None else total + term
    third = (m[9] + m[13] + m[17]) * (1.0 / 3.0)
    for i in (9, 13, 17):
        d = m[i] - third
        total = total + d * d
    return total


def kernel(
    sizes, raw_ref, time_ref, out_ref, sums_ref,
    raw_in, field, back, edge_out, edge_in, step_out, step_in, full_in,
    time_links, time_in, rotated, parts, total_out, total_in,
    raw_sems, edge_sems, step_sems, full_sems, time_sems, total_sems,
):
    n_t, n_x, n_y = sizes
    ring = n_x == 2
    offsets = (0, 1) if ring else (0, n_x - 1, 1)
    slots = len(offsets)
    ahead = [offsets.index((d + 1) % n_x) if (d + 1) % n_x in offsets else p for p, d in enumerate(offsets)]
    behind = [offsets.index((d - 1) % n_x) if (d - 1) % n_x in offsets else p for p, d in enumerate(offsets)]
    t, x, y = lax.axis_index("ta"), lax.axis_index("gx"), lax.axis_index("gy")

    def device(dt, dx, dy):
        return {
            "ta": lax.rem(t + dt % n_t, n_t),
            "gx": lax.rem(x + dx % n_x, n_x),
            "gy": lax.rem(y + dy % n_y, n_y),
        }

    def remote(src, dst, sems, index, dt, dx, dy):
        return pltpu.make_async_remote_copy(
            src_ref=src,
            dst_ref=dst,
            send_sem=sems.at[(0,) + index],
            recv_sem=sems.at[(1,) + index],
            device_id=device(dt, dx, dy),
            device_id_type=MESH,
        )

    peers = [(0, dx, dy) for dx in range(n_x) for dy in range(n_y) if dx or dy]
    greet = peers + [(1, 0, 0), (n_t - 1, 0, 0)]
    barrier = pltpu.get_barrier_semaphore()
    for peer in greet:
        pl.semaphore_signal(barrier, inc=1, device_id=device(*peer), device_id_type=MESH)

    lane = lax.broadcasted_iota(jnp.int32, (8, 128), 1)
    row = lax.broadcasted_iota(jnp.int32, (8, 128), 0)
    z = lax.rem(lane, 64)
    masks = (lane, z)
    first_plane = [lax.rem(lane + lax.div(lane, 64) + u, 2) == 0 for u in (0, 1)]
    counted = (row >= 1) & (row <= 6) & (z < NZ)

    def spread_row(ref, rows, s):
        lanes = lax.broadcasted_iota(jnp.int32, (rows, 128), 1)
        start = 2 * NZ * s
        number, off = start // 128, start % 128
        low = ref[:, number * 128 : number * 128 + 128]
        high = ref[:, number * 128 + 128 : number * 128 + 256] if off + 2 * NZ > 128 else None

        def window(shift):
            one = pltpu.roll(low, (-shift) % 128, 1)
            if high is None:
                return one
            return jnp.where(lanes + shift < 128, one, pltpu.roll(high, (-shift) % 128, 1))

        return jnp.where(lanes < 64, window(off), window(off + NZ - 64))

    rows = 2 * COMPS
    last = 6
    edge_low = spread_row(raw_ref, rows, 0)
    edge_high = spread_row(raw_ref, rows, last - 1)
    edge_out[0] = edge_low
    edge_out[1] = edge_high
    own = field.at[0]
    own[pl.ds(1, rows, stride=8), :] = edge_low
    own[pl.ds(last, rows, stride=8), :] = edge_high

    pl.semaphore_wait(barrier, len(greet))
    first_copies = []
    for p, d in enumerate(offsets):
        if d:
            first_copies.append(remote(raw_ref, raw_in.at[p - 1], raw_sems, (p - 1,), 0, -d, 0))
            first_copies[-1].start()
    edge_copies = []
    for p, d in enumerate(offsets):
        for way in (0, 1):
            edge_copies.append(
                remote(edge_out.at[way], edge_in.at[p, way], edge_sems, (p, way), 0, -d, (-1, 1)[way])
            )
            edge_copies[-1].start()

    for s in range(1, last - 1):
        own[pl.ds(s + 1, rows, stride=8), :] = spread_row(raw_ref, rows, s)
    for s in range(6):
        time_links[pl.ds(s + 1, 40, stride=8), :] = spread_row(time_ref, 40, s)
    for copy in first_copies:
        copy.wait_recv()
    for p in range(1, slots):
        for s in range(last):
            field.at[p][pl.ds(s + 1, rows, stride=8), :] = spread_row(raw_in.at[p - 1], rows, s)
    for copy in edge_copies:
        copy.wait_recv()
    for p in range(slots):
        field.at[p][pl.ds(7, rows, stride=8), :] = edge_in[p, 0]
        field.at[p][pl.ds(0, rows, stride=8), :] = edge_in[p, 1]

    def matrix(p, colour, base):
        return [tile(field.at[p], colour * COMPS + base + c) for c in range(18)]

    def neighbour(p, colour, base, c, direction, step):
        at = (1 - colour) * COMPS + base + c
        here = tile(field.at[p], at)
        if direction == 2:
            return z_shift(here, masks, step)
        if direction == 1:
            return y_shift(here, masks, step)
        if step > 0:
            return jnp.where(first_plane[colour], here, tile(field.at[ahead[p]], at))
        return jnp.where(first_plane[colour], tile(field.at[behind[p]], at), here)

    for p in range(slots):
        for direction in range(3):
            for colour in (0, 1):
                for c in range(18):
                    value = neighbour(p, colour, direction * 18, c, direction, -1)
                    back[p, pl.ds((((direction * 2) + colour) * 18 + c) * 8, 8), :] = value

    def staple(p, colour):
        total = [None] * 18
        for direction in range(3):
            u = matrix(p, colour, direction * 18)
            g = [neighbour(p, colour, GAUGE, c, direction, 1) for c in range(18)]
            add_links_times_dagger(total, u, g)
            v = [tile(back.at[p], (direction * 2 + colour) * 18 + c) for c in range(18)]
            g = [neighbour(p, colour, GAUGE, c, direction, -1) for c in range(18)]
            add_dagger_times_dagger(total, v, g)
        return total

    def half(p, colour):
        g, m = relax(matrix(p, colour, GAUGE), times(matrix(p, colour, GAUGE), staple(p, colour)))
        return g, m

    def store(p, colour, g):
        for c in range(18):
            field[p, pl.ds((colour * COMPS + GAUGE + c) * 8, 8), :] = g[c]

    summed = range(slots) if ring else range(1)

    def gauge_rows(p, colour):
        return field.at[p, pl.ds((colour * COMPS + GAUGE) * 8, 18 * 8), :]

    def time_copy(colour):
        return remote(gauge_rows(0, colour), time_in.at[colour], time_sems, (colour,), -1, 0, 0)

    def step_copies(k):
        copies = []
        if ring:
            for way in (0, 1):
                copies.append(
                    remote(
                        step_out.at[k, way], step_in.at[k, 0, way], step_sems, (k, 0, way), 0, 0, (-1, 1)[way]
                    )
                )
        else:
            for p, d in enumerate(offsets):
                for way in (0, 1):
                    copies.append(
                        remote(
                            step_out.at[k, way], step_in.at[k, p, way], step_sems, (k, p, way),
                            0, -d, (-1, 1)[way],
                        )
                    )
                if d:
                    copies.append(
                        remote(gauge_rows(0, 1), full_in.at[k, p - 1], full_sems, (k, p - 1), 0, -d, 0)
                    )
        return copies

    def iteration(k, carry):
        for p in range(slots):
            g, m = half(p, 0)
            store(p, 0, g)

        @pl.when(k == ITERS - 1)
        def _():
            time_copy(0).start()

        trace = None
        square = None
        for p in range(slots):
            g, m = half(p, 1)
            store(p, 1, g)
            if p in summed:
                one = m[0] + m[4] + m[8]
                trace = one if trace is None else trace + one
                two = squares(m)
                square = two if square is None else square + two
        parts[k] = jnp.where(counted, trace, 0.0)
        parts[ITERS] = jnp.where(counted, square, 0.0)
        base = (COMPS + GAUGE) * 8
        for p in summed:
            for way in (0, 1):
                edge = field.at[p][pl.ds(base + (1, last)[way], 18, stride=8), :]
                step_out[k, way, p] = edge
        copies = step_copies(k)
        for copy in copies:
            copy.start()

        for copy in copies:
            copy.wait_send()
        for copy in copies:
            copy.wait_recv()
        if not ring:
            for p in range(1, slots):
                field[p, pl.ds(base, 144), :] = full_in[k, p - 1]
        for p in range(slots):
            source = (0, p) if ring else (p, 0)
            field.at[p][pl.ds(base + 7, 18, stride=8), :] = step_in[k, source[0], 0, source[1]]
            field.at[p][pl.ds(base, 18, stride=8), :] = step_in[k, source[0], 1, source[1]]
        return carry

    lax.fori_loop(0, ITERS, iteration, 0)
    time_copy(1).start()

    square = None
    for p in summed:
        two = squares(times(matrix(p, 0, GAUGE), staple(p, 0)))
        square = two if square is None else square + two
    parts[ITERS] = parts[ITERS] + jnp.where(counted, square, 0.0)
    block = jnp.zeros((8, 128), jnp.float32)
    for k in range(ITERS + 1):
        block = block + jnp.where(row == k, jnp.sum(parts[k], axis=0, keepdims=True), 0.0)
    total_out[...] = block
    group = [(0, 0, dy) for dy in range(1, n_y)] if ring else peers
    me = y if ring else x * n_y + y
    total_in[me] = block
    total_copies = [
        remote(total_out, total_in.at[me], total_sems, (number,), 0, dx, dy)
        for number, (_, dx, dy) in enumerate(group)
    ]
    for copy in total_copies:
        copy.start()

    def emit(which, ref, first_row):
        for colour in (0, 1):
            pieces = []
            lanes = lax.broadcasted_iota(jnp.int32, (18, 128), 1)
            for s in range(6):
                v = ref[pl.ds(first_row(colour) * 8 + s + 1, 18, stride=8), :]
                pieces.append(jnp.where(lanes < NZ, v, pltpu.roll(v, 128 - (64 - NZ), 1)))
            for number in range(5):
                value = None
                for s in range(6):
                    start = 2 * NZ * s - 128 * number
                    if start >= 128 or start + 2 * NZ <= 0:
                        continue
                    moved = pltpu.roll(pieces[s], start % 128, 1) if start % 128 else pieces[s]
                    value = moved if value is None else jnp.where(lanes >= start, moved, value)
                out_ref[which, colour, :, number * 128 : number * 128 + 128] = value

    emit(0, field.at[0], lambda colour: colour * COMPS + GAUGE)
    for colour in (0, 1):
        time_copy(colour).wait_recv()
    for colour in (0, 1):
        v = [tile(time_links, colour * 18 + c) for c in range(18)]
        g = [tile(time_in.at[colour], c) for c in range(18)]
        turned = [None] * 18
        add_links_times_dagger(turned, times(matrix(0, colour, GAUGE), v), g)
        for c in range(18):
            rotated[pl.ds((colour * 18 + c) * 8, 8), :] = turned[c]
    emit(1, rotated, lambda colour: colour * 18)

    for copy in first_copies + edge_copies + total_copies:
        copy.wait_send()
    for colour in (0, 1):
        time_copy(colour).wait_send()
    for copy in total_copies:
        copy.wait_recv()
    total = total_in[0]
    for number in range(1, len(group) + 1):
        total = total + total_in[number]
    sums_ref[...] = jnp.broadcast_to(jnp.sum(total, axis=1, keepdims=True), (8, 128))


def local(space_links, time_links, start_gauge):
    n_t, n_x, n_y = (lax.axis_size(a) for a in ("ta", "gx", "gy"))
    planes, width = start_gauge.shape[4], start_gauge.shape[5]
    assert start_gauge.shape[3] == 1 and planes == 2 and width == 12 * NZ
    volume = planes * n_x * width * n_y
    ring = n_x == 2
    slots = 2 if ring else 3
    group = n_y if ring else n_x * n_y
    site = jnp.arange(width)
    even = (site // NZ + site % NZ) % 2 == 0

    def packed(a):
        a = a.reshape((-1, planes, width))
        low, high = a[:, 0], a[:, 1]
        return jnp.where(even, low, high), jnp.where(even, high, low)

    links = packed(space_links)
    gauge = packed(start_gauge)
    times_ = packed(time_links)
    wide = (-width) % 128
    raw = jnp.pad(
        jnp.concatenate([links[0], gauge[0], links[1], gauge[1]], axis=0), ((0, 0), (0, wide))
    )
    temporal = jnp.pad(jnp.concatenate(times_, axis=0), ((0, 4), (0, wide)))
    vmem = pl.BlockSpec(memory_space=pltpu.VMEM)
    f32 = jnp.float32
    dma = pltpu.SemaphoreType.DMA
    n_full = 1 if ring else ITERS
    out, sums = pl.pallas_call(
        functools.partial(kernel, (n_t, n_x, n_y)),
        out_shape=(
            jax.ShapeDtypeStruct((2, 2, 18, width + wide), f32),
            jax.ShapeDtypeStruct((8, 128), f32),
        ),
        in_specs=[vmem, vmem],
        out_specs=(vmem, vmem),
        scratch_shapes=[
            pltpu.VMEM((slots - 1, 2 * COMPS, width + wide), f32),
            pltpu.VMEM((slots, 2 * COMPS * 8, 128), f32),
            pltpu.VMEM((slots, 108 * 8, 128), f32),
            pltpu.VMEM((2, 2 * COMPS, 128), f32),
            pltpu.VMEM((slots, 2, 2 * COMPS, 128), f32),
            pltpu.VMEM((ITERS, 2, 2 if ring else 1, 18, 128), f32),
            pltpu.VMEM((ITERS, 1 if ring else 3, 2, 2 if ring else 1, 18, 128), f32),
            pltpu.VMEM((n_full, 2, 144, 128), f32),
            pltpu.VMEM((40 * 8, 128), f32),
            pltpu.VMEM((2, 144, 128), f32),
            pltpu.VMEM((288, 128), f32),
            pltpu.VMEM((ITERS + 1, 8, 128), f32),
            pltpu.VMEM((8, 128), f32),
            pltpu.VMEM((group, 8, 128), f32),
            dma((2, slots - 1)),
            dma((2, slots, 2)),
            dma((2, ITERS, 1 if ring else 3, 2)),
            dma((2, n_full, 2)),
            dma((2, 2)),
            dma((2, group - 1)),
        ],
        compiler_params=pltpu.CompilerParams(collective_id=0, has_side_effects=True),
    )(raw, temporal)

    def unpacked(a):
        first, second = a[0, :, :width], a[1, :, :width]
        both = jnp.stack([jnp.where(even, first, second), jnp.where(even, second, first)], axis=1)
        return both.reshape((2, 3, 3, 1, planes, width))

    functional = sums[:ITERS, :1] / (9.0 * volume)
    theta = sums[ITERS, :1] / (3.0 * volume)
    return (unpacked(out[0]), unpacked(out[1]), functional, theta)


def solution(mesh):
    field = P(None, None, None, "ta", "gx", "gy")
    return jax.shard_map(
        local,
        mesh=mesh,
        in_specs=(P(None, None, None, None, "ta", "gx", "gy"), field, field),
        out_specs=(field, field, P(None, "ta"), P("ta")),
        check_vma=False,
    )
```

```python
import functools

import jax
import jax.numpy as jnp
from jax import lax
from jax.experimental import pallas as pl
from jax.experimental.pallas import tpu as pltpu
from jax.sharding import PartitionSpec as P

NZ = 48
ITERS = 4
OMEGA = 1.7
FLOOR = 0.5
PAIRS = ((0, 1), (1, 2), (0, 2))

SENT = 48
MESH = pl.DeviceIdType.MESH


def tile(ref, row):
    return ref[pl.ds(row * 8, 8), :]


def z_shift(v, masks, step):
    lane, z = masks
    if step > 0:
        return jnp.where(z == NZ - 1, pltpu.roll(v, NZ - 1, 1), pltpu.roll(v, 127, 1))
    return jnp.where(z == 0, pltpu.roll(v, 128 - (NZ - 1), 1), pltpu.roll(v, 1, 1))


def y_shift(v, masks, step):
    lane, z = masks
    swapped = pltpu.roll(v, 64, 1)
    if step > 0:
        return jnp.where(lane < 64, swapped, pltpu.roll(swapped, 7, 0))
    return jnp.where(lane >= 64, swapped, pltpu.roll(swapped, 1, 0))


def add_links_times_dagger(total, u, g):
    for i in range(3):
        for j in range(3):
            re, im = total[i * 3 + j], total[9 + i * 3 + j]
            for k in range(3):
                ur, ui = u[i * 3 + k], u[9 + i * 3 + k]
                gr, gi = g[j * 3 + k], g[9 + j * 3 + k]
                tr = ur * gr + ui * gi
                ti = ui * gr - ur * gi
                re = tr if re is None else re + tr
                im = ti if im is None else im + ti
            total[i * 3 + j], total[9 + i * 3 + j] = re, im


def add_dagger_times_dagger(total, v, g):
    for i in range(3):
        for j in range(3):
            re, im = total[i * 3 + j], total[9 + i * 3 + j]
            for k in range(3):
                vr, vi = v[k * 3 + i], v[9 + k * 3 + i]
                gr, gi = g[j * 3 + k], g[9 + j * 3 + k]
                tr = vr * gr - vi * gi
                ti = vr * gi + vi * gr
                re = tr if re is None else re + tr
                im = -ti if im is None else im - ti
            total[i * 3 + j], total[9 + i * 3 + j] = re, im


def times(a, b):
    out = [None] * 18
    for i in range(3):
        for j in range(3):
            re = im = None
            for k in range(3):
                ar, ai = a[i * 3 + k], a[9 + i * 3 + k]
                br, bi = b[k * 3 + j], b[9 + k * 3 + j]
                tr = ar * br - ai * bi
                ti = ar * bi + ai * br
                re = tr if re is None else re + tr
                im = ti if im is None else im + ti
            out[i * 3 + j], out[9 + i * 3 + j] = re, im
    return out


def turn(m, i, j, a):
    out = list(m)
    for col in range(3):
        fr, fi = m[i * 3 + col], m[9 + i * 3 + col]
        sr, si = m[j * 3 + col], m[9 + j * 3 + col]
        out[i * 3 + col] = (a[0] * fr - a[3] * fi) + (a[2] * sr - a[1] * si)
        out[9 + i * 3 + col] = (a[0] * fi + a[3] * fr) + (a[2] * si + a[1] * sr)
        out[j * 3 + col] = (a[0] * sr + a[3] * si) - (a[2] * fr + a[1] * fi)
        out[9 + j * 3 + col] = (a[0] * si - a[3] * sr) - (a[2] * fi - a[1] * fr)
    return out


def relax(g, m):
    for i, j in PAIRS:
        c0 = m[i * 3 + i] + m[j * 3 + j]
        c1 = -(m[9 + i * 3 + j] + m[9 + j * 3 + i])
        c2 = m[j * 3 + i] - m[i * 3 + j]
        c3 = m[9 + j * 3 + j] - m[9 + i * 3 + i]
        length = jnp.sqrt(c0 * c0 + c1 * c1 + c2 * c2 + c3 * c3)
        v0 = (1.0 - OMEGA) * length + OMEGA * c0
        v1, v2, v3 = OMEGA * c1, OMEGA * c2, OMEGA * c3
        inverse = jnp.minimum(lax.rsqrt(v0 * v0 + v1 * v1 + v2 * v2 + v3 * v3), 1.0 / FLOOR)
        a = [v0 * inverse, v1 * inverse, v2 * inverse, v3 * inverse]
        g = turn(g, i, j, a)
        m = turn(m, i, j, a)
    return g, m


def squares(m):
    total = None
    for i, j in ((0, 1), (0, 2), (1, 2)):
        a = m[i * 3 + j] - m[j * 3 + i]
        b = m[9 + i * 3 + j] + m[9 + j * 3 + i]
        term = 0.5 * (a * a + b * b)
        total = term if total is None else total + term
    third = (m[9] + m[13] + m[17]) * (1.0 / 3.0)
    for i in (9, 13, 17):
        d = m[i] - third
        total = total + d * d
    return total


def kernel(
    sizes, links_ref, gauge_ref, time_ref, out_ref, sums_ref,
    raw, flat, time_raw, time_flat, field, gauge, back, edge_out, edge_in, step_out, step_in, full_in,
    time_links, time_in, rotated, parts, total_out, total_in,
    local_sems, raw_sems, edge_sems, step_sems, full_sems, time_sems, total_sems,
):
    n_t, n_x, n_y = sizes
    ring = n_x == 2
    offsets = (0, 1) if ring else (0, n_x - 1, 1)
    slots = len(offsets)
    ahead = [offsets.index((d + 1) % n_x) if (d + 1) % n_x in offsets else p for p, d in enumerate(offsets)]
    behind = [offsets.index((d - 1) % n_x) if (d - 1) % n_x in offsets else p for p, d in enumerate(offsets)]
    t, x, y = lax.axis_index("ta"), lax.axis_index("gx"), lax.axis_index("gy")

    def device(dt, dx, dy):
        return {
            "ta": lax.rem(t + dt % n_t, n_t),
            "gx": lax.rem(x + dx % n_x, n_x),
            "gy": lax.rem(y + dy % n_y, n_y),
        }

    def remote(src, dst, sems, index, dt, dx, dy):
        return pltpu.make_async_remote_copy(
            src_ref=src,
            dst_ref=dst,
            send_sem=sems.at[(0,) + index],
            recv_sem=sems.at[(1,) + index],
            device_id=device(dt, dx, dy),
            device_id_type=MESH,
        )

    local_copies = [
        pltpu.make_async_copy(links_ref.at[:, pl.ds(0, 6)], raw.at[0, pl.ds(0, 6)], local_sems.at[0]),
        pltpu.make_async_copy(gauge_ref.at[:, pl.ds(0, 6)], raw.at[0, pl.ds(6, 2)], local_sems.at[1]),
        pltpu.make_async_copy(time_ref, time_raw, local_sems.at[2]),
    ]
    for copy in local_copies:
        copy.start()
    peers = [(0, dx, dy) for dx in range(n_x) for dy in range(n_y) if dx or dy]
    group = [(0, 0, dy) for dy in range(1, n_y)] if ring else peers
    near = [(0, d, dy) for d in offsets for dy in (0, 1, n_y - 1) if d or dy]
    greet = sorted(set(group + near + [(1, 0, 0), (n_t - 1, 0, 0)]))
    barrier = pltpu.get_barrier_semaphore()
    for peer in greet:
        pl.semaphore_signal(barrier, inc=1, device_id=device(*peer), device_id_type=MESH)

    lane = lax.broadcasted_iota(jnp.int32, (8, 128), 1)
    row = lax.broadcasted_iota(jnp.int32, (8, 128), 0)
    z = lax.rem(lane, 64)
    masks = (lane, z)
    first_plane = [lax.rem(lane + lax.div(lane, 64) + u, 2) == 0 for u in (0, 1)]
    counted = (row >= 1) & (row <= 6) & (z < NZ)

    def spread_row(ref, rows, s):
        lanes = lax.broadcasted_iota(jnp.int32, (rows, 128), 1)
        start = 2 * NZ * s
        number, off = start // 128, start % 128
        low = ref[:, number * 128 : number * 128 + 128]
        high = ref[:, number * 128 + 128 : number * 128 + 256] if off + 2 * NZ > 128 else None

        def window(shift):
            one = pltpu.roll(low, (-shift) % 128, 1)
            if high is None:
                return one
            return jnp.where(lanes + shift < 128, one, pltpu.roll(high, (-shift) % 128, 1))

        return jnp.where(lanes < 64, window(off), window(off + NZ - 64))

    rows = 2 * SENT
    last = 6

    def flatten(source, target, count):
        for number in range(5):
            lanes = min(128, 12 * NZ - 128 * number)
            at = slice(128 * number, 128 * number + lanes)
            site = 128 * number + lax.broadcasted_iota(jnp.int32, (count, 128), 1)
            even = lax.rem(lax.div(site, NZ) + lax.rem(site, NZ), 2) == 0
            planes = [source[:, plane, at] for plane in (0, 1)]
            if lanes < 128:
                planes = [jnp.concatenate([v, v], axis=1) for v in planes]
            whole = slice(128 * number, 128 * number + 128)
            target[0:count, whole] = jnp.where(even, planes[0], planes[1])
            target[count : 2 * count, whole] = jnp.where(even, planes[1], planes[0])

    pl.semaphore_wait(barrier, len(greet))
    first_copies = []
    for p, d in enumerate(offsets):
        if d:
            first_copies.append(
                remote(
                    gauge_ref.at[:, pl.ds(0, 6)], raw.at[p, pl.ds(6, 2)], raw_sems, (p - 1, 1), 0, -d, 0
                )
            )
            first_copies.append(
                remote(
                    links_ref.at[:, pl.ds(0, 6)], raw.at[p, pl.ds(0, 6)], raw_sems, (p - 1, 0), 0, -d, 0
                )
            )
    for copy in local_copies:
        copy.wait()
    own = field.at[0]
    flatten(raw.at[0].reshape(SENT, 2, 12 * NZ), flat, SENT)
    for way, s in ((0, 0), (1, last - 1)):
        edge = spread_row(flat, rows, s)
        edge_out[way] = edge
        own[pl.ds(s + 1, rows, stride=8), :] = edge
    edge_copies = []
    for p, d in enumerate(offsets):
        for way in (0, 1):
            edge_copies.append(
                remote(edge_out.at[way], edge_in.at[p, way], edge_sems, (p, way), 0, -d, (-1, 1)[way])
            )
            edge_copies[-1].start()
    for copy in first_copies:
        copy.start()

    for s in range(1, last - 1):
        own[pl.ds(s + 1, rows, stride=8), :] = spread_row(flat, rows, s)
    flatten(time_raw, time_flat, 18)
    for s in range(6):
        time_links[pl.ds(s + 1, 36, stride=8), :] = spread_row(time_flat, 36, s)
    for copy in first_copies:
        copy.wait_recv()
    for p in range(1, slots):
        flatten(raw.at[p].reshape(SENT, 2, 12 * NZ), flat, SENT)
        for s in range(last):
            field.at[p][pl.ds(s + 1, rows, stride=8), :] = spread_row(flat, rows, s)
    for copy in edge_copies:
        copy.wait_recv()
    for p in range(slots):
        field.at[p][pl.ds(7, rows, stride=8), :] = edge_in[p, 0]
        field.at[p][pl.ds(0, rows, stride=8), :] = edge_in[p, 1]

    def link_row(colour, which, c):
        part, inner = divmod(c, 9)
        if inner < 6:
            return colour * SENT + (which * 2 + part) * 6 + inner
        return rows + colour * 18 + (which * 2 + part) * 3 + inner - 6

    def put(ref, p, at, value):
        ref[p, pl.ds(at * 8, 8), :] = value

    for p in range(slots):
        for colour in (0, 1):
            for which in range(4):
                m = [None] * 18
                for c in range(18):
                    if c % 9 < 6:
                        m[c] = tile(field.at[p], link_row(colour, which, c))
                for k in range(3):
                    i, j = (k + 1) % 3, (k + 2) % 3
                    ar, ai, br, bi = m[i], m[9 + i], m[3 + j], m[12 + j]
                    cr, ci, dr, di = m[j], m[9 + j], m[3 + i], m[12 + i]
                    m[6 + k] = (ar * br - ai * bi) - (cr * dr - ci * di)
                    m[15 + k] = (cr * di + ci * dr) - (ar * bi + ai * br)
                for c in range(18):
                    if which == 3:
                        put(gauge, p, colour * 18 + c, m[c])
                    elif c % 9 >= 6:
                        put(field, p, link_row(colour, which, c), m[c])

    def links(p, colour, which):
        return [tile(field.at[p], link_row(colour, which, c)) for c in range(18)]

    def matrix(p, colour):
        return [tile(gauge.at[p], colour * 18 + c) for c in range(18)]

    def neighbour(ref, p, colour, at, direction, step):
        here = tile(ref.at[p], at)
        if direction == 2:
            return z_shift(here, masks, step)
        if direction == 1:
            return y_shift(here, masks, step)
        if step > 0:
            return jnp.where(first_plane[colour], here, tile(ref.at[ahead[p]], at))
        return jnp.where(first_plane[colour], tile(ref.at[behind[p]], at), here)

    for p in range(slots):
        for direction in range(3):
            for colour in (0, 1):
                for c in range(18):
                    value = neighbour(
                        field, p, colour, link_row(1 - colour, direction, c), direction, -1
                    )
                    put(back, p, (direction * 2 + colour) * 18 + c, value)

    def around(p, colour, direction, step):
        return [
            neighbour(gauge, p, colour, (1 - colour) * 18 + c, direction, step) for c in range(18)
        ]

    def staple(p, colour):
        total = [None] * 18
        for direction in range(3):
            u = links(p, colour, direction)
            g = around(p, colour, direction, 1)
            add_links_times_dagger(total, u, g)
            v = [tile(back.at[p], (direction * 2 + colour) * 18 + c) for c in range(18)]
            g = around(p, colour, direction, -1)
            add_dagger_times_dagger(total, v, g)
        return total

    def half(p, colour):
        g, m = relax(matrix(p, colour), times(matrix(p, colour), staple(p, colour)))
        return g, m

    def store(p, colour, g):
        for c in range(18):
            put(gauge, p, colour * 18 + c, g[c])

    summed = range(slots) if ring else range(1)

    def gauge_rows(p, colour):
        return gauge.at[p, pl.ds(colour * 144, 144), :]

    def time_copy(colour):
        return remote(gauge_rows(0, colour), time_in.at[colour], time_sems, (colour,), -1, 0, 0)

    def step_copies(k):
        copies = []
        if ring:
            for way in (0, 1):
                copies.append(
                    remote(
                        step_out.at[k, way], step_in.at[k, 0, way], step_sems, (k, 0, way), 0, 0, (-1, 1)[way]
                    )
                )
        else:
            for p, d in enumerate(offsets):
                for way in (0, 1):
                    copies.append(
                        remote(
                            step_out.at[k, way], step_in.at[k, p, way], step_sems, (k, p, way),
                            0, -d, (-1, 1)[way],
                        )
                    )
                if d:
                    copies.append(
                        remote(gauge_rows(0, 1), full_in.at[k, p - 1], full_sems, (k, p - 1), 0, -d, 0)
                    )
        return copies

    def iteration(k, carry):
        for p in range(slots):
            g, m = half(p, 0)
            store(p, 0, g)

        @pl.when(k == ITERS - 1)
        def _():
            time_copy(0).start()

        trace = None
        square = None
        for p in range(slots):
            g, m = half(p, 1)
            store(p, 1, g)
            if p in summed:
                one = m[0] + m[4] + m[8]
                trace = one if trace is None else trace + one
                two = squares(m)
                square = two if square is None else square + two
        parts[k] = jnp.where(counted, trace, 0.0)
        parts[ITERS] = jnp.where(counted, square, 0.0)
        base = 144
        for p in summed:
            for way in (0, 1):
                edge = gauge.at[p][pl.ds(base + (1, last)[way], 18, stride=8), :]
                step_out[k, way, p] = edge
        copies = step_copies(k)
        for copy in copies:
            copy.start()

        for copy in copies:
            copy.wait_send()
        for copy in copies:
            copy.wait_recv()
        if not ring:
            for p in range(1, slots):
                gauge[p, pl.ds(base, 144), :] = full_in[k, p - 1]
        for p in range(slots):
            source = (0, p) if ring else (p, 0)
            gauge.at[p][pl.ds(base + 7, 18, stride=8), :] = step_in[k, source[0], 0, source[1]]
            gauge.at[p][pl.ds(base, 18, stride=8), :] = step_in[k, source[0], 1, source[1]]
        return carry

    lax.fori_loop(0, ITERS, iteration, 0)
    time_copy(1).start()

    square = None
    for p in summed:
        two = squares(times(matrix(p, 0), staple(p, 0)))
        square = two if square is None else square + two
    parts[ITERS] = parts[ITERS] + jnp.where(counted, square, 0.0)
    block = jnp.zeros((8, 128), jnp.float32)
    for k in range(ITERS + 1):
        block = block + jnp.where(row == k, jnp.sum(parts[k], axis=0, keepdims=True), 0.0)
    total_out[...] = block
    me = y if ring else x * n_y + y
    total_in[me] = block
    total_copies = [
        remote(total_out, total_in.at[me], total_sems, (number,), 0, dx, dy)
        for number, (_, dx, dy) in enumerate(group)
    ]
    for copy in total_copies:
        copy.start()

    def emit(which, ref, first_row):
        for colour in (0, 1):
            pieces = []
            lanes = lax.broadcasted_iota(jnp.int32, (18, 128), 1)
            for s in range(6):
                v = ref[pl.ds(first_row(colour) * 8 + s + 1, 18, stride=8), :]
                pieces.append(jnp.where(lanes < NZ, v, pltpu.roll(v, 128 - (64 - NZ), 1)))
            for number in range(5):
                value = None
                for s in range(6):
                    start = 2 * NZ * s - 128 * number
                    if start >= 128 or start + 2 * NZ <= 0:
                        continue
                    moved = pltpu.roll(pieces[s], start % 128, 1) if start % 128 else pieces[s]
                    value = moved if value is None else jnp.where(lanes >= start, moved, value)
                out_ref[which, colour, :, number * 128 : number * 128 + 128] = value

    emit(0, gauge.at[0], lambda colour: colour * 18)
    for colour in (0, 1):
        time_copy(colour).wait_recv()
    for colour in (0, 1):
        v = [tile(time_links, colour * 18 + c) for c in range(18)]
        g = [tile(time_in.at[colour], c) for c in range(18)]
        turned = [None] * 18
        add_links_times_dagger(turned, times(matrix(0, colour), v), g)
        for c in range(18):
            rotated[pl.ds((colour * 18 + c) * 8, 8), :] = turned[c]
    emit(1, rotated, lambda colour: colour * 18)

    for copy in first_copies + edge_copies + total_copies:
        copy.wait_send()
    for colour in (0, 1):
        time_copy(colour).wait_send()
    for copy in total_copies:
        copy.wait_recv()
    total = total_in[0]
    for number in range(1, len(group) + 1):
        total = total + total_in[number]
    sums_ref[...] = jnp.broadcast_to(jnp.sum(total, axis=1, keepdims=True), (8, 128))


def finish(volume, packed_ref, sums_ref, gauge_ref, time_ref, functional_ref, theta_ref):
    for which, ref in enumerate((gauge_ref, time_ref)):
        for number in range(5):
            lanes = min(128, 12 * NZ - 128 * number)
            at = slice(128 * number, 128 * number + lanes)
            site = 128 * number + lax.broadcasted_iota(jnp.int32, (18, lanes), 1)
            even = lax.rem(lax.div(site, NZ) + lax.rem(site, NZ), 2) == 0
            first, second = (packed_ref[which, colour, :, at] for colour in (0, 1))
            ref[:, 0, at] = jnp.where(even, first, second)
            ref[:, 1, at] = jnp.where(even, second, first)
    lane = lax.broadcasted_iota(jnp.int32, (8, 128), 1)
    row = lax.broadcasted_iota(jnp.int32, (8, 128), 0)
    along = jnp.sum(jnp.where(lane == row, sums_ref[...], 0.0), axis=0, keepdims=True)
    functional_ref[...] = along[:, :ITERS] * (1.0 / (9.0 * volume))
    theta_ref[...] = sums_ref[ITERS : ITERS + 1, 0:1] * (1.0 / (3.0 * volume))


def local(space_links, time_links, start_gauge):
    n_t, n_x, n_y = (lax.axis_size(a) for a in ("ta", "gx", "gy"))
    planes, width = start_gauge.shape[4], start_gauge.shape[5]
    assert start_gauge.shape[3] == 1 and planes == 2 and width == 12 * NZ
    volume = planes * n_x * width * n_y
    ring = n_x == 2
    slots = 2 if ring else 3
    group = n_y if ring else n_x * n_y
    wide = width + (-width) % 128
    vmem = pl.BlockSpec(memory_space=pltpu.VMEM)
    anywhere = pl.BlockSpec(memory_space=pl.ANY)
    f32 = jnp.float32
    dma = pltpu.SemaphoreType.DMA
    n_full = 1 if ring else ITERS
    packed, sums = pl.pallas_call(
        functools.partial(kernel, (n_t, n_x, n_y)),
        out_shape=(
            jax.ShapeDtypeStruct((2, 2, 18, wide), f32),
            jax.ShapeDtypeStruct((8, 128), f32),
        ),
        in_specs=[anywhere] * 3,
        out_specs=(vmem, vmem),
        scratch_shapes=[
            pltpu.VMEM((slots, 8, 6, planes, width), f32),
            pltpu.VMEM((2 * SENT, wide), f32),
            pltpu.VMEM((18, planes, width), f32),
            pltpu.VMEM((36, wide), f32),
            pltpu.VMEM((slots, (2 * SENT + 36) * 8, 128), f32),
            pltpu.VMEM((slots, 36 * 8, 128), f32),
            pltpu.VMEM((slots, 108 * 8, 128), f32),
            pltpu.VMEM((2, 2 * SENT, 128), f32),
            pltpu.VMEM((slots, 2, 2 * SENT, 128), f32),
            pltpu.VMEM((ITERS, 2, 2 if ring else 1, 18, 128), f32),
            pltpu.VMEM((ITERS, 1 if ring else 3, 2, 2 if ring else 1, 18, 128), f32),
            pltpu.VMEM((n_full, 2, 144, 128), f32),
            pltpu.VMEM((36 * 8, 128), f32),
            pltpu.VMEM((2, 144, 128), f32),
            pltpu.VMEM((288, 128), f32),
            pltpu.VMEM((ITERS + 1, 8, 128), f32),
            pltpu.VMEM((8, 128), f32),
            pltpu.VMEM((group, 8, 128), f32),
            dma((3,)),
            dma((2, slots - 1, 2)),
            dma((2, slots, 2)),
            dma((2, ITERS, 1 if ring else 3, 2)),
            dma((2, n_full, 2)),
            dma((2, 2)),
            dma((2, group - 1)),
        ],
        compiler_params=pltpu.CompilerParams(collective_id=0, has_side_effects=True),
    )(
        space_links.reshape((6, 9, planes, width)),
        start_gauge.reshape((2, 9, planes, width)),
        time_links.reshape((18, planes, width)),
    )
    gauge, rotated, functional, theta = pl.pallas_call(
        functools.partial(finish, volume),
        out_shape=(
            jax.ShapeDtypeStruct((18, planes, width), f32),
            jax.ShapeDtypeStruct((18, planes, width), f32),
            jax.ShapeDtypeStruct((1, ITERS), f32),
            jax.ShapeDtypeStruct((1, 1), f32),
        ),
        in_specs=[vmem, vmem],
        out_specs=(vmem,) * 4,
    )(packed, sums)
    shape = start_gauge.shape
    return (
        gauge.reshape(shape),
        rotated.reshape(shape),
        functional.reshape((ITERS, 1)),
        theta.reshape((1,)),
    )


def solution(mesh):
    field = P(None, None, None, "ta", "gx", "gy")
    return jax.shard_map(
        local,
        mesh=mesh,
        in_specs=(P(None, None, None, None, "ta", "gx", "gy"), field, field),
        out_specs=(field, field, P(None, "ta"), P("ta")),
        check_vma=False,
    )
```

```python
import functools

import jax
import jax.numpy as jnp
from jax import lax
from jax.experimental import pallas as pl
from jax.experimental.pallas import tpu as pltpu
from jax.sharding import PartitionSpec as P

NZ = 48
ITERS = 4
OMEGA = 1.7
FLOOR = 0.5
PAIRS = ((0, 1), (1, 2), (0, 2))

SENT = 48
MESH = pl.DeviceIdType.MESH


def tile(ref, row):
    return ref[pl.ds(row * 8, 8), :]


def z_shift(v, masks, step):
    lane, z = masks
    if step > 0:
        return jnp.where(z == NZ - 1, pltpu.roll(v, NZ - 1, 1), pltpu.roll(v, 127, 1))
    return jnp.where(z == 0, pltpu.roll(v, 128 - (NZ - 1), 1), pltpu.roll(v, 1, 1))


def y_shift(v, masks, step):
    lane, z = masks
    swapped = pltpu.roll(v, 64, 1)
    if step > 0:
        return jnp.where(lane < 64, swapped, pltpu.roll(swapped, 7, 0))
    return jnp.where(lane >= 64, swapped, pltpu.roll(swapped, 1, 0))


def add_links_times_dagger(total, u, g):
    for i in range(3):
        for j in range(3):
            re, im = total[i * 3 + j], total[9 + i * 3 + j]
            for k in range(3):
                ur, ui = u[i * 3 + k], u[9 + i * 3 + k]
                gr, gi = g[j * 3 + k], g[9 + j * 3 + k]
                tr = ur * gr + ui * gi
                ti = ui * gr - ur * gi
                re = tr if re is None else re + tr
                im = ti if im is None else im + ti
            total[i * 3 + j], total[9 + i * 3 + j] = re, im


def add_dagger_times_dagger(total, v, g):
    for i in range(3):
        for j in range(3):
            re, im = total[i * 3 + j], total[9 + i * 3 + j]
            for k in range(3):
                vr, vi = v[k * 3 + i], v[9 + k * 3 + i]
                gr, gi = g[j * 3 + k], g[9 + j * 3 + k]
                tr = vr * gr - vi * gi
                ti = vr * gi + vi * gr
                re = tr if re is None else re + tr
                im = -ti if im is None else im - ti
            total[i * 3 + j], total[9 + i * 3 + j] = re, im


def times(a, b):
    out = [None] * 18
    for i in range(3):
        for j in range(3):
            re = im = None
            for k in range(3):
                ar, ai = a[i * 3 + k], a[9 + i * 3 + k]
                br, bi = b[k * 3 + j], b[9 + k * 3 + j]
                tr = ar * br - ai * bi
                ti = ar * bi + ai * br
                re = tr if re is None else re + tr
                im = ti if im is None else im + ti
            out[i * 3 + j], out[9 + i * 3 + j] = re, im
    return out


def turn(m, i, j, a):
    out = list(m)
    for col in range(3):
        fr, fi = m[i * 3 + col], m[9 + i * 3 + col]
        sr, si = m[j * 3 + col], m[9 + j * 3 + col]
        out[i * 3 + col] = (a[0] * fr - a[3] * fi) + (a[2] * sr - a[1] * si)
        out[9 + i * 3 + col] = (a[0] * fi + a[3] * fr) + (a[2] * si + a[1] * sr)
        out[j * 3 + col] = (a[0] * sr + a[3] * si) - (a[2] * fr + a[1] * fi)
        out[9 + j * 3 + col] = (a[0] * si - a[3] * sr) - (a[2] * fi - a[1] * fr)
    return out


def relax(g, m):
    for i, j in PAIRS:
        c0 = m[i * 3 + i] + m[j * 3 + j]
        c1 = -(m[9 + i * 3 + j] + m[9 + j * 3 + i])
        c2 = m[j * 3 + i] - m[i * 3 + j]
        c3 = m[9 + j * 3 + j] - m[9 + i * 3 + i]
        length = jnp.sqrt(c0 * c0 + c1 * c1 + c2 * c2 + c3 * c3)
        v0 = (1.0 - OMEGA) * length + OMEGA * c0
        v1, v2, v3 = OMEGA * c1, OMEGA * c2, OMEGA * c3
        inverse = jnp.minimum(lax.rsqrt(v0 * v0 + v1 * v1 + v2 * v2 + v3 * v3), 1.0 / FLOOR)
        a = [v0 * inverse, v1 * inverse, v2 * inverse, v3 * inverse]
        g = turn(g, i, j, a)
        m = turn(m, i, j, a)
    return g, m


def squares(m):
    total = None
    for i, j in ((0, 1), (0, 2), (1, 2)):
        a = m[i * 3 + j] - m[j * 3 + i]
        b = m[9 + i * 3 + j] + m[9 + j * 3 + i]
        term = 0.5 * (a * a + b * b)
        total = term if total is None else total + term
    third = (m[9] + m[13] + m[17]) * (1.0 / 3.0)
    for i in (9, 13, 17):
        d = m[i] - third
        total = total + d * d
    return total


def kernel(
    sizes, links_ref, gauge_ref, time_ref, out_ref, sums_ref,
    raw, flat, time_raw, time_flat, field, gauge, back, edge_out, edge_in, step_out, step_in, full_in,
    time_links, time_in, rotated, parts, total_out, total_in,
    local_sems, raw_sems, edge_sems, step_sems, full_sems, time_sems, total_sems,
):
    n_t, n_x, n_y = sizes
    ring = n_x == 2
    offsets = (0, 1) if ring else (0, n_x - 1, 1)
    slots = len(offsets)
    ahead = [offsets.index((d + 1) % n_x) if (d + 1) % n_x in offsets else p for p, d in enumerate(offsets)]
    behind = [offsets.index((d - 1) % n_x) if (d - 1) % n_x in offsets else p for p, d in enumerate(offsets)]
    t, x, y = lax.axis_index("ta"), lax.axis_index("gx"), lax.axis_index("gy")

    def device(dt, dx, dy):
        return {
            "ta": lax.rem(t + dt % n_t, n_t),
            "gx": lax.rem(x + dx % n_x, n_x),
            "gy": lax.rem(y + dy % n_y, n_y),
        }

    def remote(src, dst, sems, index, dt, dx, dy):
        return pltpu.make_async_remote_copy(
            src_ref=src,
            dst_ref=dst,
            send_sem=sems.at[(0,) + index],
            recv_sem=sems.at[(1,) + index],
            device_id=device(dt, dx, dy),
            device_id_type=MESH,
        )

    local_copies = [
        pltpu.make_async_copy(links_ref.at[:, pl.ds(0, 6)], raw.at[0, pl.ds(0, 6)], local_sems.at[0]),
        pltpu.make_async_copy(gauge_ref.at[:, pl.ds(0, 6)], raw.at[0, pl.ds(6, 2)], local_sems.at[1]),
        pltpu.make_async_copy(time_ref, time_raw, local_sems.at[2]),
    ]
    for copy in local_copies:
        copy.start()
    peers = [(0, dx, dy) for dx in range(n_x) for dy in range(n_y) if dx or dy]
    group = [(0, 0, dy) for dy in range(1, n_y)] if ring else peers
    near = [(0, d, dy) for d in offsets for dy in (0, 1, n_y - 1) if d or dy]
    greet = sorted(set(group + near + [(1, 0, 0), (n_t - 1, 0, 0)]))
    barrier = pltpu.get_barrier_semaphore()
    for peer in greet:
        pl.semaphore_signal(barrier, inc=1, device_id=device(*peer), device_id_type=MESH)

    lane = lax.broadcasted_iota(jnp.int32, (8, 128), 1)
    row = lax.broadcasted_iota(jnp.int32, (8, 128), 0)
    z = lax.rem(lane, 64)
    masks = (lane, z)
    first_plane = [lax.rem(lane + lax.div(lane, 64) + u, 2) == 0 for u in (0, 1)]
    counted = (row >= 1) & (row <= 6) & (z < NZ)

    def spread_row(ref, rows, s):
        lanes = lax.broadcasted_iota(jnp.int32, (rows, 128), 1)
        start = 2 * NZ * s
        number, off = start // 128, start % 128
        low = ref[:, number * 128 : number * 128 + 128]
        high = ref[:, number * 128 + 128 : number * 128 + 256] if off + 2 * NZ > 128 else None

        def window(shift):
            one = pltpu.roll(low, (-shift) % 128, 1)
            if high is None:
                return one
            return jnp.where(lanes + shift < 128, one, pltpu.roll(high, (-shift) % 128, 1))

        return jnp.where(lanes < 64, window(off), window(off + NZ - 64))

    rows = 2 * SENT
    last = 6

    def flatten(source, target, count):
        for number in range(5):
            lanes = min(128, 12 * NZ - 128 * number)
            at = slice(128 * number, 128 * number + lanes)
            site = 128 * number + lax.broadcasted_iota(jnp.int32, (count, 128), 1)
            even = lax.rem(lax.div(site, NZ) + lax.rem(site, NZ), 2) == 0
            planes = [source[:, plane, at] for plane in (0, 1)]
            if lanes < 128:
                planes = [jnp.concatenate([v, v], axis=1) for v in planes]
            whole = slice(128 * number, 128 * number + 128)
            target[0:count, whole] = jnp.where(even, planes[0], planes[1])
            target[count : 2 * count, whole] = jnp.where(even, planes[1], planes[0])

    first_copies = []
    for p, d in enumerate(offsets):
        if d:
            first_copies.append(
                remote(
                    gauge_ref.at[:, pl.ds(0, 6)], raw.at[p, pl.ds(6, 2)], raw_sems, (p - 1, 1), 0, -d, 0
                )
            )
            first_copies.append(
                remote(
                    links_ref.at[:, pl.ds(0, 6)], raw.at[p, pl.ds(0, 6)], raw_sems, (p - 1, 0), 0, -d, 0
                )
            )
    for copy in local_copies:
        copy.wait()
    own = field.at[0]
    flatten(raw.at[0].reshape(SENT, 2, 12 * NZ), flat, SENT)
    for way, s in ((0, 0), (1, last - 1)):
        edge = spread_row(flat, rows, s)
        edge_out[way] = edge
        own[pl.ds(s + 1, rows, stride=8), :] = edge
    pl.semaphore_wait(barrier, len(greet))
    edge_copies = []
    for p, d in enumerate(offsets):
        for way in (0, 1):
            edge_copies.append(
                remote(edge_out.at[way], edge_in.at[p, way], edge_sems, (p, way), 0, -d, (-1, 1)[way])
            )
            edge_copies[-1].start()
    for copy in first_copies:
        copy.start()

    for s in range(1, last - 1):
        own[pl.ds(s + 1, rows, stride=8), :] = spread_row(flat, rows, s)
    flatten(time_raw, time_flat, 18)
    for s in range(6):
        time_links[pl.ds(s + 1, 36, stride=8), :] = spread_row(time_flat, 36, s)
    for copy in first_copies:
        copy.wait_recv()
    for p in range(1, slots):
        flatten(raw.at[p].reshape(SENT, 2, 12 * NZ), flat, SENT)
        for s in range(last):
            field.at[p][pl.ds(s + 1, rows, stride=8), :] = spread_row(flat, rows, s)
    for copy in edge_copies:
        copy.wait_recv()
    for p in range(slots):
        field.at[p][pl.ds(7, rows, stride=8), :] = edge_in[p, 0]
        field.at[p][pl.ds(0, rows, stride=8), :] = edge_in[p, 1]

    def link_row(colour, which, c):
        part, inner = divmod(c, 9)
        if inner < 6:
            return colour * SENT + (which * 2 + part) * 6 + inner
        return rows + colour * 18 + (which * 2 + part) * 3 + inner - 6

    def put(ref, p, at, value):
        ref[p, pl.ds(at * 8, 8), :] = value

    for p in range(slots):
        for colour in (0, 1):
            for which in range(4):
                m = [None] * 18
                for c in range(18):
                    if c % 9 < 6:
                        m[c] = tile(field.at[p], link_row(colour, which, c))
                for k in range(3):
                    i, j = (k + 1) % 3, (k + 2) % 3
                    ar, ai, br, bi = m[i], m[9 + i], m[3 + j], m[12 + j]
                    cr, ci, dr, di = m[j], m[9 + j], m[3 + i], m[12 + i]
                    m[6 + k] = (ar * br - ai * bi) - (cr * dr - ci * di)
                    m[15 + k] = (cr * di + ci * dr) - (ar * bi + ai * br)
                for c in range(18):
                    if which == 3:
                        put(gauge, p, colour * 18 + c, m[c])
                    elif c % 9 >= 6:
                        put(field, p, link_row(colour, which, c), m[c])

    def links(p, colour, which):
        return [tile(field.at[p], link_row(colour, which, c)) for c in range(18)]

    def matrix(p, colour):
        return [tile(gauge.at[p], colour * 18 + c) for c in range(18)]

    def neighbour(ref, p, colour, at, direction, step):
        here = tile(ref.at[p], at)
        if direction == 2:
            return z_shift(here, masks, step)
        if direction == 1:
            return y_shift(here, masks, step)
        if step > 0:
            return jnp.where(first_plane[colour], here, tile(ref.at[ahead[p]], at))
        return jnp.where(first_plane[colour], tile(ref.at[behind[p]], at), here)

    for p in range(slots):
        for direction in range(3):
            for colour in (0, 1):
                for c in range(18):
                    value = neighbour(
                        field, p, colour, link_row(1 - colour, direction, c), direction, -1
                    )
                    put(back, p, (direction * 2 + colour) * 18 + c, value)

    def around(p, colour, direction, step):
        return [
            neighbour(gauge, p, colour, (1 - colour) * 18 + c, direction, step) for c in range(18)
        ]

    def staple(p, colour):
        total = [None] * 18
        for direction in range(3):
            u = links(p, colour, direction)
            g = around(p, colour, direction, 1)
            add_links_times_dagger(total, u, g)
            v = [tile(back.at[p], (direction * 2 + colour) * 18 + c) for c in range(18)]
            g = around(p, colour, direction, -1)
            add_dagger_times_dagger(total, v, g)
        return total

    def half(p, colour):
        g, m = relax(matrix(p, colour), times(matrix(p, colour), staple(p, colour)))
        return g, m

    def store(p, colour, g):
        for c in range(18):
            put(gauge, p, colour * 18 + c, g[c])

    summed = range(slots) if ring else range(1)

    def gauge_rows(p, colour):
        return gauge.at[p, pl.ds(colour * 144, 144), :]

    def time_copy(colour):
        return remote(gauge_rows(0, colour), time_in.at[colour], time_sems, (colour,), -1, 0, 0)

    def step_copies(k, q):
        copies = []
        if ring:
            for way in (0, 1):
                copies.append(
                    remote(
                        step_out.at[k, way, q], step_in.at[k, 0, way, q], step_sems, (k, q, way),
                        0, 0, (-1, 1)[way],
                    )
                )
        else:
            for p, d in enumerate(offsets):
                for way in (0, 1):
                    copies.append(
                        remote(
                            step_out.at[k, way], step_in.at[k, p, way], step_sems, (k, p, way),
                            0, -d, (-1, 1)[way],
                        )
                    )
                if d:
                    copies.append(
                        remote(gauge_rows(0, 1), full_in.at[k, p - 1], full_sems, (k, p - 1), 0, -d, 0)
                    )
        return copies

    def iteration(k, carry):
        for p in range(slots):
            g, m = half(p, 0)
            store(p, 0, g)

        @pl.when(k == ITERS - 1)
        def _():
            time_copy(0).start()

        trace = None
        square = None
        base = 144
        copies = []
        for p in range(slots):
            g, m = half(p, 1)
            store(p, 1, g)
            if p in summed:
                for way in (0, 1):
                    edge = gauge.at[p][pl.ds(base + (1, last)[way], 18, stride=8), :]
                    step_out[k, way, p] = edge
                started = step_copies(k, p)
                for copy in started:
                    copy.start()
                copies += started
            if p in summed:
                one = m[0] + m[4] + m[8]
                trace = one if trace is None else trace + one
                two = squares(m)
                square = two if square is None else square + two
        parts[k] = jnp.where(counted, trace, 0.0)
        parts[ITERS] = jnp.where(counted, square, 0.0)
        for copy in copies:
            copy.wait_send()
        for copy in copies:
            copy.wait_recv()
        if not ring:
            for p in range(1, slots):
                gauge[p, pl.ds(base, 144), :] = full_in[k, p - 1]
        for p in range(slots):
            source = (0, p) if ring else (p, 0)
            gauge.at[p][pl.ds(base + 7, 18, stride=8), :] = step_in[k, source[0], 0, source[1]]
            gauge.at[p][pl.ds(base, 18, stride=8), :] = step_in[k, source[0], 1, source[1]]
        return carry

    lax.fori_loop(0, ITERS, iteration, 0)
    time_copy(1).start()

    square = None
    for p in summed:
        two = squares(times(matrix(p, 0), staple(p, 0)))
        square = two if square is None else square + two
    parts[ITERS] = parts[ITERS] + jnp.where(counted, square, 0.0)
    block = jnp.zeros((8, 128), jnp.float32)
    for k in range(ITERS + 1):
        block = block + jnp.where(row == k, jnp.sum(parts[k], axis=0, keepdims=True), 0.0)
    total_out[...] = block
    me = y if ring else x * n_y + y
    total_in[me] = block
    total_copies = [
        remote(total_out, total_in.at[me], total_sems, (number,), 0, dx, dy)
        for number, (_, dx, dy) in enumerate(group)
    ]
    for copy in total_copies:
        copy.start()

    def emit(which, ref, first_row):
        for colour in (0, 1):
            pieces = []
            lanes = lax.broadcasted_iota(jnp.int32, (18, 128), 1)
            for s in range(6):
                v = ref[pl.ds(first_row(colour) * 8 + s + 1, 18, stride=8), :]
                pieces.append(jnp.where(lanes < NZ, v, pltpu.roll(v, 128 - (64 - NZ), 1)))
            for number in range(5):
                value = None
                for s in range(6):
                    start = 2 * NZ * s - 128 * number
                    if start >= 128 or start + 2 * NZ <= 0:
                        continue
                    moved = pltpu.roll(pieces[s], start % 128, 1) if start % 128 else pieces[s]
                    value = moved if value is None else jnp.where(lanes >= start, moved, value)
                out_ref[which, colour, :, number * 128 : number * 128 + 128] = value

    emit(0, gauge.at[0], lambda colour: colour * 18)
    for colour in (0, 1):
        time_copy(colour).wait_recv()
    for colour in (0, 1):
        v = [tile(time_links, colour * 18 + c) for c in range(18)]
        g = [tile(time_in.at[colour], c) for c in range(18)]
        turned = [None] * 18
        add_links_times_dagger(turned, times(matrix(0, colour), v), g)
        for c in range(18):
            rotated[pl.ds((colour * 18 + c) * 8, 8), :] = turned[c]
    emit(1, rotated, lambda colour: colour * 18)

    for copy in first_copies + edge_copies + total_copies:
        copy.wait_send()
    for colour in (0, 1):
        time_copy(colour).wait_send()
    for copy in total_copies:
        copy.wait_recv()
    total = total_in[0]
    for number in range(1, len(group) + 1):
        total = total + total_in[number]
    sums_ref[...] = jnp.broadcast_to(jnp.sum(total, axis=1, keepdims=True), (8, 128))


def finish(volume, packed_ref, sums_ref, gauge_ref, time_ref, functional_ref, theta_ref):
    for which, ref in enumerate((gauge_ref, time_ref)):
        for number in range(5):
            lanes = min(128, 12 * NZ - 128 * number)
            at = slice(128 * number, 128 * number + lanes)
            site = 128 * number + lax.broadcasted_iota(jnp.int32, (18, lanes), 1)
            even = lax.rem(lax.div(site, NZ) + lax.rem(site, NZ), 2) == 0
            first, second = (packed_ref[which, colour, :, at] for colour in (0, 1))
            ref[:, 0, at] = jnp.where(even, first, second)
            ref[:, 1, at] = jnp.where(even, second, first)
    lane = lax.broadcasted_iota(jnp.int32, (8, 128), 1)
    row = lax.broadcasted_iota(jnp.int32, (8, 128), 0)
    along = jnp.sum(jnp.where(lane == row, sums_ref[...], 0.0), axis=0, keepdims=True)
    functional_ref[...] = along[:, :ITERS] * (1.0 / (9.0 * volume))
    theta_ref[...] = sums_ref[ITERS : ITERS + 1, 0:1] * (1.0 / (3.0 * volume))


def local(space_links, time_links, start_gauge):
    n_t, n_x, n_y = (lax.axis_size(a) for a in ("ta", "gx", "gy"))
    planes, width = start_gauge.shape[4], start_gauge.shape[5]
    assert start_gauge.shape[3] == 1 and planes == 2 and width == 12 * NZ
    volume = planes * n_x * width * n_y
    ring = n_x == 2
    slots = 2 if ring else 3
    group = n_y if ring else n_x * n_y
    wide = width + (-width) % 128
    vmem = pl.BlockSpec(memory_space=pltpu.VMEM)
    anywhere = pl.BlockSpec(memory_space=pl.ANY)
    f32 = jnp.float32
    dma = pltpu.SemaphoreType.DMA
    n_full = 1 if ring else ITERS
    packed, sums = pl.pallas_call(
        functools.partial(kernel, (n_t, n_x, n_y)),
        out_shape=(
            jax.ShapeDtypeStruct((2, 2, 18, wide), f32),
            jax.ShapeDtypeStruct((8, 128), f32),
        ),
        in_specs=[anywhere] * 3,
        out_specs=(vmem, vmem),
        scratch_shapes=[
            pltpu.VMEM((slots, 8, 6, planes, width), f32),
            pltpu.VMEM((2 * SENT, wide), f32),
            pltpu.VMEM((18, planes, width), f32),
            pltpu.VMEM((36, wide), f32),
            pltpu.VMEM((slots, (2 * SENT + 36) * 8, 128), f32),
            pltpu.VMEM((slots, 36 * 8, 128), f32),
            pltpu.VMEM((slots, 108 * 8, 128), f32),
            pltpu.VMEM((2, 2 * SENT, 128), f32),
            pltpu.VMEM((slots, 2, 2 * SENT, 128), f32),
            pltpu.VMEM((ITERS, 2, 2 if ring else 1, 18, 128), f32),
            pltpu.VMEM((ITERS, 1 if ring else 3, 2, 2 if ring else 1, 18, 128), f32),
            pltpu.VMEM((n_full, 2, 144, 128), f32),
            pltpu.VMEM((36 * 8, 128), f32),
            pltpu.VMEM((2, 144, 128), f32),
            pltpu.VMEM((288, 128), f32),
            pltpu.VMEM((ITERS + 1, 8, 128), f32),
            pltpu.VMEM((8, 128), f32),
            pltpu.VMEM((group, 8, 128), f32),
            dma((3,)),
            dma((2, slots - 1, 2)),
            dma((2, slots, 2)),
            dma((2, ITERS, slots, 2)),
            dma((2, n_full, 2)),
            dma((2, 2)),
            dma((2, group - 1)),
        ],
        compiler_params=pltpu.CompilerParams(collective_id=0, has_side_effects=True),
    )(
        space_links.reshape((6, 9, planes, width)),
        start_gauge.reshape((2, 9, planes, width)),
        time_links.reshape((18, planes, width)),
    )
    gauge, rotated, functional, theta = pl.pallas_call(
        functools.partial(finish, volume),
        out_shape=(
            jax.ShapeDtypeStruct((18, planes, width), f32),
            jax.ShapeDtypeStruct((18, planes, width), f32),
            jax.ShapeDtypeStruct((1, ITERS), f32),
            jax.ShapeDtypeStruct((1, 1), f32),
        ),
        in_specs=[vmem, vmem],
        out_specs=(vmem,) * 4,
    )(packed, sums)
    shape = start_gauge.shape
    return (
        gauge.reshape(shape),
        rotated.reshape(shape),
        functional.reshape((ITERS, 1)),
        theta.reshape((1,)),
    )


def solution(mesh):
    field = P(None, None, None, "ta", "gx", "gy")
    return jax.shard_map(
        local,
        mesh=mesh,
        in_specs=(P(None, None, None, None, "ta", "gx", "gy"), field, field),
        out_specs=(field, field, P(None, "ta"), P("ta")),
        check_vma=False,
    )
```
